1024 devices in a mesh: comp: 2 (over core), blk: 512 (over y, z, x).
Axes of the slice: x: 8, y: 8, z: 8, core: 2. Of those that a mesh axis runs over, the one named last changes fastest.
Arguments:
- initial: float32 [2, 5, 4096, 2048], P('comp', None, 'blk'), may hold values from -3 to 3
- ice_forcing: float32 [5, 4096, 2048], P(None, 'blk'), may hold values from -2 to 4, as said below
- ocean_current: float32 [2, 4096, 2048], P(None, 'blk'), may hold values from -1 to 1
- ice_cover: int32 [4096, 2048], P('blk'), may hold values from 0 to 1, as said below
- targets: int32 [2, 4096, 2048], P(None, 'blk'), may hold values from 0 to 32767, as said below
- weights: int32 [2, 4096, 2048], P(None, 'blk'), may hold values from 1 to 4
Outputs:
- state_out: float32 [2, 5, 4096, 2048], P('comp', None, 'blk')
- coupled: float32 [2, 3, 4096, 2048], P('comp', None, 'blk')
The draws below stay inside these ranges and needn't reach their ends.
Inputs may be any that keep to these rules, and one draw needn't show every extreme that they name: `ice_forcing`: channel 0 (mass) lies in 0.5 to 4, channel 1 (strength) and channel 4 (melt rate) in 0.2 to 2, channels 2 and 3 (wind stress) in -2 to 2. `ice_cover`: the share of ice-covered cells differs from strip to strip of 8 rows. `targets`: an entry of an ice cell at row r of its strip names an ocean row of the window no earlier than r.
All inputs are finite; a program needn't handle non-finite values.
Results may differ from the reference program's by a relative error of at most 0.0003.
Values sent between devices are 32-bit elements; how exact they have to be, the bound alone decides.
A program may use at most 128 MiB of HBM per device.

```python
import math
import jax
import jax.numpy as jnp
from jax import lax

CX = 8
NY = 2048
SUBCYCLES = 16
INTERSECTIONS = 2
NX = 4096


def smooth_field(key, channels):
    row_pos = jnp.arange(NX, dtype=jnp.float32)[None, :, None]
    col_pos = jnp.arange(NY, dtype=jnp.float32)[None, None, :]
    summed = jnp.zeros((channels, NX, NY), jnp.float32)
    for wave_index in range(3):
        wave_key = jax.random.fold_in(key, 100 + wave_index)
        picks = jax.random.uniform(wave_key, (3, channels), jnp.float32)
        row_length = jnp.exp(math.log(48.0) + (math.log(160.0) - math.log(48.0)) * picks[0])[:, None, None]
        col_length = jnp.exp(math.log(32.0) + (math.log(512.0) - math.log(32.0)) * picks[1])[:, None, None]
        summed = summed + jnp.sin(2.0 * math.pi * (row_pos / row_length + col_pos / col_length + picks[2][:, None, None]))
    return summed / 2.0


def draw_initial(key, part):
    smooth = smooth_field(jax.random.fold_in(key, 31), 10).reshape(2, 5, NX, NY)
    noise = jax.random.normal(jax.random.fold_in(key, 32), (2, 5, NX, NY), jnp.float32)
    values = 0.8 * smooth + 0.35 * noise
    return jnp.clip(values, -3.0, 3.0).astype(jnp.float32)


def draw_ice_forcing(key, part):
    shape = (NX, NY)
    keys = jax.random.split(key, 5)
    smooth = smooth_field(jax.random.fold_in(key, 51), 2)
    mass = jnp.exp(jax.random.uniform(keys[0], shape, jnp.float32, math.log(0.5), math.log(4.0)))
    strength = jnp.exp(jax.random.uniform(keys[1], shape, jnp.float32, math.log(0.2), math.log(2.0)))
    wind_x = jnp.clip(0.6 * smooth[0] + 0.3 * jax.random.normal(keys[2], shape, jnp.float32), -2.0, 2.0)
    wind_y = jnp.clip(0.6 * smooth[1] + 0.3 * jax.random.normal(keys[3], shape, jnp.float32), -2.0, 2.0)
    melt = jnp.exp(jax.random.uniform(keys[4], shape, jnp.float32, math.log(0.2), math.log(2.0)))
    return jnp.stack([mass, strength, wind_x, wind_y, melt]).astype(jnp.float32)


def draw_ocean_current(key, part):
    smooth = smooth_field(jax.random.fold_in(key, 41), 2)
    noise = jax.random.uniform(jax.random.fold_in(key, 42), (2, NX, NY), jnp.float32, -1.0, 1.0)
    along = 0.6 * jnp.tanh(3.0 * smooth[0]) + 0.35 * noise[0]
    sideways = 0.5 * smooth[1] + 0.4 * noise[1]
    return jnp.clip(jnp.stack([along, sideways]), -1.0, 1.0).astype(jnp.float32)


def draw_ice_cover(key, part):
    level = jnp.minimum(jax.random.randint(jax.random.fold_in(key, 11), (NX // CX,), 0, 24), 8)
    cells = jax.random.randint(jax.random.fold_in(key, 12), (NX, NY), 0, 8)
    strip = jnp.arange(NX, dtype=jnp.int32) // CX
    return (cells < level[strip][:, None]).astype(jnp.int32)


def draw_targets(key, part):
    offset = jax.random.randint(jax.random.fold_in(key, 21), (INTERSECTIONS, NX, NY), 0, CX + 1)
    jitter = jax.random.randint(jax.random.fold_in(key, 22), (INTERSECTIONS, NX, NY), -2, 3)
    local_row = (jnp.arange(NX, dtype=jnp.int32) % CX)[None, :, None]
    column = jnp.arange(NY, dtype=jnp.int32)[None, None, :]
    return ((local_row + offset) * NY + (column + jitter) % NY).astype(jnp.int32)


def with_ends(array, stream_key, least, high):
    place = [jax.random.randint(jax.random.fold_in(stream_key, axis), (), 0, length) for axis, length in enumerate(array.shape)]
    main_axis = array.shape.index(max(array.shape))
    beside = place[:main_axis] + [(place[main_axis] + 1) % array.shape[main_axis]] + place[main_axis + 1:]
    return array.at[tuple(place)].set(least).at[tuple(beside)].set(high)


def setup_inputs(seed: int = 0) -> dict:
    key_list = jax.random.split(jax.random.key(seed), 7)
    initial = draw_initial(jax.random.fold_in(key_list[6], 71), 0)
    ice_forcing = draw_ice_forcing(jax.random.fold_in(key_list[6], 71), 0)
    ocean_current = draw_ocean_current(jax.random.fold_in(key_list[6], 71), 0)
    ice_cover = draw_ice_cover(jax.random.fold_in(key_list[6], 71), 0)
    targets = draw_targets(jax.random.fold_in(key_list[6], 71), 0)
    weights = with_ends(jax.random.randint(key_list[5], (INTERSECTIONS, NX, NY), 1, 5), jax.random.fold_in(key_list[5], 1), 1, 4).astype(jnp.int32)
    return dict(initial=initial, ice_forcing=ice_forcing, ocean_current=ocean_current, ice_cover=ice_cover, targets=targets, weights=weights)


relax_rate = 0.5
ecc_sq = 4.0
delta_floor = 0.1
coriolis = 0.1
drag_coef = 1.0
inertia = 4.0
courant = 0.2
dilution = 0.5
weight_norm = 4.0
level_speed = (1.0, 0.8, 0.6, 0.45, 0.3)

def along_rows(field):
    return 0.5 * (field[..., 2:, :] - field[..., :-2, :])

def across(field):
    padded = jnp.pad(field, [(0, 0)] * (field.ndim - 1) + [(1, 1)])
    return 0.5 * (padded[..., 2:] - padded[..., :-2])

def ice_step(fields, forcing, current, covered):
    vel_x = fields[0]
    vel_y = fields[1]
    strain_d = along_rows(vel_x) + across(vel_y[1:-1])
    strain_t = along_rows(vel_x) - across(vel_y[1:-1])
    strain_s = across(vel_x[1:-1]) + along_rows(vel_y)
    delta = jnp.sqrt(strain_d * strain_d + (strain_t * strain_t + strain_s * strain_s) / ecc_sq + delta_floor * delta_floor)
    press = forcing[1, 1:-1] * covered[1:-1]
    sig_one = (fields[2, 1:-1] + relax_rate * press * (strain_d / delta - 1.0)) / (1.0 + relax_rate)
    sig_two = (fields[3, 1:-1] + relax_rate * press * strain_t / (ecc_sq * delta)) / (1.0 + relax_rate)
    sig_shear = (fields[4, 1:-1] + relax_rate * press * strain_s / (2.0 * ecc_sq * delta)) / (1.0 + relax_rate)
    sig_xx = 0.5 * (sig_one + sig_two)
    sig_yy = 0.5 * (sig_one - sig_two)
    force_x = along_rows(sig_xx) + across(sig_shear[1:-1])
    force_y = along_rows(sig_shear) + across(sig_yy[1:-1])
    beta = inertia * forcing[0, 2:-2]
    old_x = vel_x[2:-2]
    old_y = vel_y[2:-2]
    denom = beta + drag_coef
    new_x = covered[2:-2] * (beta * old_x + coriolis * beta * old_y + force_x + forcing[2, 2:-2] + drag_coef * current[0, 2:-2]) / denom
    new_y = covered[2:-2] * (beta * old_y - coriolis * beta * old_x + force_y + forcing[3, 2:-2] + drag_coef * current[1, 2:-2]) / denom
    return jnp.stack([new_x, new_y, sig_one[1:-1], sig_two[1:-1], sig_shear[1:-1]])

def ocean_step(tracer, current):
    speed = jnp.asarray(level_speed, jnp.float32)[:, None, None]
    centre = tracer[:, 2:-2]
    below = centre - tracer[:, 1:-3]
    above = tracer[:, 3:-1] - centre
    padded = jnp.pad(centre, ((0, 0), (0, 0), (1, 1)))
    left_diff = centre - padded[:, :, :-2]
    right_diff = padded[:, :, 2:] - centre
    speed_x = speed * current[0, 2:-2][None]
    speed_y = speed * current[1, 2:-2][None]
    change = jnp.maximum(speed_x, 0.0) * below + jnp.minimum(speed_x, 0.0) * above + jnp.maximum(speed_y, 0.0) * left_diff + jnp.minimum(speed_y, 0.0) * right_diff
    return centre - courant * change

def coupling_terms(fields, forcing, current, covered):
    stress_x = covered * drag_coef * (fields[0] - current[0])
    stress_y = covered * drag_coef * (fields[1] - current[1])
    fresh = forcing[4] * covered * jnp.sqrt(1.0 + fields[0] * fields[0] + fields[1] * fields[1])
    return jnp.stack([stress_x, stress_y, fresh])

def pad_rows(values):
    return jnp.pad(values, [(0, 0)] * (values.ndim - 2) + [(2, 2), (0, 0)])

def reference(initial, ice_forcing, ocean_current, ice_cover, targets, weights):
    covered = ice_cover.astype(jnp.float32)
    forcing_pad = pad_rows(ice_forcing)
    current_pad = pad_rows(ocean_current)
    cover_pad = pad_rows(covered)

    def one_turn(carry, unused):
        ice_fields, salinity, total = carry
        ice_fields = ice_step(pad_rows(ice_fields), forcing_pad, current_pad, cover_pad)
        salinity = ocean_step(pad_rows(salinity), current_pad)
        total = total + coupling_terms(ice_fields, ice_forcing, ocean_current, covered)
        return ((ice_fields, salinity, total), None)
    start = (initial[0], initial[1], jnp.zeros((3, NX, NY), jnp.float32))
    (ice_fields, salinity, total), unused = lax.scan(one_turn, start, None, length=SUBCYCLES)
    average = total / SUBCYCLES
    row_index = jnp.arange(NX, dtype=jnp.int32)[:, None]
    base = row_index // CX * (CX * NY)
    glob = (targets + base[None]) % (NX * NY)
    scaled = weights.astype(jnp.float32) / weight_norm
    flat_glob = glob.reshape(-1)

    def spread(single):
        return jax.ops.segment_sum((single[None] * scaled).reshape(-1), flat_glob, num_segments=NX * NY)
    flux = jax.vmap(spread)(average).reshape(3, NX, NY)
    salinity = jnp.concatenate([salinity[:1] - dilution * flux[2][None], salinity[1:]], axis=0)
    state_out = jnp.stack([ice_fields, salinity])
    coupled = jnp.stack([average, flux])
    return (state_out, coupled)
```

```python
import functools
import jax
import jax.numpy as jnp
from jax import lax
from jax.experimental import pallas as pl
from jax.experimental.pallas import tpu as pltpu
from jax.sharding import PartitionSpec as P

LEVELS = (1.0, 0.8, 0.6, 0.45, 0.3)
OWN = 8
RB = 32
LANE = 128
MESH = pl.DeviceIdType.MESH
UP, DOWN = 0, 1


def own(ref, *lead):
    return ref.at[lead + (slice(None),) * (len(ref.shape) - 2 - len(lead)) + (pl.ds(OWN, 8), slice(None))]


def kernel(n, nt, init, forcing, current, cover, targets, weights, state_out, coupled_out,
           S, W, T, F, CUR, COV, TG, WT, TOT, VALS, TH, TL, ACC, FLUX, RECVW, RECVA,
           load_sem, send_sem, recv_sem, st_send, st_recv, a_send, a_recv, w_send, w_recv, out_sem, gate):
    comp = lax.axis_index("comp")
    b = lax.axis_index("blk")
    is_ice = comp == 0
    has_up = b > 0
    has_down = b < n - 1
    nxt = lax.rem(b + 1, n)
    prv = lax.rem(b + n - 1, n)

    loads = [
        pltpu.make_async_copy(init, S.at[0, :, :, pl.ds(OWN, 8), :], load_sem.at[0]),
        pltpu.make_async_copy(forcing, F, load_sem.at[1]),
        pltpu.make_async_copy(current, CUR.at[:, :, pl.ds(OWN, 8), :], load_sem.at[2]),
        pltpu.make_async_copy(cover, COV, load_sem.at[3]),
        pltpu.make_async_copy(targets, TG, load_sem.at[4]),
        pltpu.make_async_copy(weights, WT, load_sem.at[5]),
    ]
    for c in loads:
        c.start()

    def zero_halo(lo):
        z5 = jnp.zeros((5, nt, 8, LANE), jnp.float32)
        for q in range(2):
            S[q, :, :, pl.ds(lo, 8), :] = z5
        T[:, :, pl.ds(lo, 8), :] = z5
        CUR[:, :, pl.ds(lo, 8), :] = jnp.zeros((2, nt, 8, LANE), jnp.float32)

    @pl.when(jnp.logical_not(has_up))
    def _():
        zero_halo(0)

    @pl.when(jnp.logical_not(has_down))
    def _():
        zero_halo(16)

    z5 = jnp.zeros((5, nt, 8, LANE), jnp.float32)
    for q in range(2):
        S[q, :, :, pl.ds(24, 8), :] = z5
    T[:, :, pl.ds(24, 8), :] = z5
    W[:, :, pl.ds(0, 8), :] = z5
    W[:, :, pl.ds(24, 8), :] = z5
    CUR[:, :, pl.ds(24, 8), :] = jnp.zeros((2, nt, 8, LANE), jnp.float32)
    TOT[...] = jnp.zeros((3, nt, 8, LANE), jnp.float32)

    barrier = pltpu.get_barrier_semaphore()

    @pl.when(has_up)
    def _():
        pl.semaphore_signal(barrier, inc=1, device_id=(comp, b - 1), device_id_type=MESH)

    @pl.when(has_down)
    def _():
        pl.semaphore_signal(barrier, inc=1, device_id=(comp, b + 1), device_id_type=MESH)

    pl.semaphore_signal(barrier, inc=1, device_id=(1 - comp, b), device_id_type=MESH)

    @pl.when(is_ice)
    def _():
        pl.semaphore_signal(barrier, inc=1, device_id=(1, nxt), device_id_type=MESH)

    @pl.when(jnp.logical_not(is_ice))
    def _():
        pl.semaphore_signal(barrier, inc=1, device_id=(0, prv), device_id_type=MESH)

    pl.semaphore_wait(barrier, 2 + has_up.astype(jnp.int32) + has_down.astype(jnp.int32))

    def remote(src, dst, ss, rs, dev):
        return pltpu.make_async_remote_copy(src_ref=src, dst_ref=dst, send_sem=ss, recv_sem=rs,
                                            device_id=dev, device_id_type=MESH)

    def state_copy(d, q, src=None):
        src = S.at[q, :, :, pl.ds(OWN, 8), :] if src is None else src
        lo, dev = (16, (comp, b - 1)) if d == UP else (0, (comp, b + 1))
        return remote(src, S.at[q, :, :, pl.ds(lo, 8), :], send_sem.at[d, q], recv_sem.at[d, q], dev)

    def ice_static_copy(d):
        lo, dev = (16, (comp, b - 1)) if d == UP else (0, (comp, b + 1))
        return remote(T.at[pl.ds(0, 4), :, pl.ds(OWN, 8), :], T.at[pl.ds(0, 4), :, pl.ds(lo, 8), :],
                      st_send.at[d], st_recv.at[d], dev)

    def ocean_static_copy(d):
        lo, dev = (16, (comp, b - 1)) if d == UP else (0, (comp, b + 1))
        return remote(current, CUR.at[:, :, pl.ds(lo, 8), :], st_send.at[d], st_recv.at[d], dev)

    def both(make, what):
        pairs = ((UP, has_up, has_down), (DOWN, has_down, has_up))
        for d, sends, receives in pairs:
            @pl.when(receives if what == "recv" else sends)
            def _():
                c = make(d)
                if what == "start":
                    c.start()
                elif what == "recv":
                    c.wait_recv()
                else:
                    c.wait_send()

    lane = lax.broadcasted_iota(jnp.int32, (nt, 8, LANE), 2)
    first = lane == 0
    last = lane == LANE - 1
    zt = jnp.zeros((1, 8, LANE), jnp.float32)

    def right_of(x):
        u = pltpu.roll(x, LANE - 1, 2)
        return jnp.where(last, jnp.concatenate([u[1:], zt], 0), u)

    def left_of(x):
        u = pltpu.roll(x, 1, 2)
        return jnp.where(first, jnp.concatenate([zt, u[:-1]], 0), u)

    def dcol(x):
        return right_of(x) - left_of(x)

    avg_copy = remote(TOT, RECVA, a_send, a_recv, (1, b))
    win_copy = remote(FLUX, RECVW, w_send, w_recv, (1, nxt))

    def scatter(avg_ref, base):
        for k in range(2):
            t = TG[k]
            row = lax.shift_right_logical(t, 11) - base
            cell = lax.bitwise_and(lax.shift_right_logical(t, 8), 7) * 8 + row
            inside = jnp.logical_and(row >= 0, row < 8)
            TH[k] = jnp.where(inside, cell, 255).astype(jnp.float32)
            TL[k] = lax.bitwise_and(t, 255).astype(jnp.float32)
            w = WT[k].astype(jnp.float32) * 0.25
            for ch in range(3):
                v = avg_ref[ch] * w
                hi = v.astype(jnp.bfloat16).astype(jnp.float32)
                VALS[k, 2 * ch] = hi
                VALS[k, 2 * ch + 1] = v - hi
        ACC[...] = jnp.zeros_like(ACC)
        iota = lax.broadcasted_iota(jnp.int32, (16, LANE), 0).astype(jnp.float32)

        def rows16(ref, k, *idx):
            return jnp.broadcast_to(ref[(k,) + idx], (16, LANE)).astype(jnp.bfloat16)

        zero = jnp.zeros((16, LANE), jnp.bfloat16)
        one = jnp.ones((16, LANE), jnp.bfloat16)
        iotas = [(iota + 16.0 * g).astype(jnp.bfloat16) for g in range(16)]

        def body(i, carry):
            k = i // 8
            r = i % 8
            total = None
            for jj in range(nt // 2):
                lhs_halves, rhs_halves = [], []
                for j in (2 * jj, 2 * jj + 1):
                    th = rows16(TH, k, j, pl.ds(r, 1), slice(None))
                    tl = rows16(TL, k, j, pl.ds(r, 1), slice(None))
                    masks = [th == iotas[g] for g in range(4)]
                    parts = []
                    for m in range(6):
                        v = rows16(VALS, k, m, j, pl.ds(r, 1), slice(None))
                        parts += [jnp.where(masks[g], v, zero) for g in range(4)]
                    lhs_halves.append(jnp.concatenate(parts, 0))
                    rhs_halves.append(jnp.concatenate([jnp.where(tl == iotas[g], one, zero) for g in range(16)], 0))
                lhs = jnp.concatenate(lhs_halves, 1)
                rhs = jnp.concatenate(rhs_halves, 1)
                part = lax.dot_general(lhs, rhs, (((1,), (1,)), ((), ())), preferred_element_type=jnp.float32)
                total = part if total is None else total + part
            ACC[...] += total
            return carry

        lax.fori_loop(0, 16, body, 0)
        for ch in range(3):
            for cb in range(nt // 2):
                for h in range(2):
                    FLUX[ch, 2 * cb + h] = (
                        ACC[pl.ds((2 * ch) * 64 + 8 * cb, 8), pl.ds(LANE * h, LANE)]
                        + ACC[pl.ds((2 * ch + 1) * 64 + 8 * cb, 8), pl.ds(LANE * h, LANE)]
                    )

    out_state = pltpu.make_async_copy(S.at[0, :, :, pl.ds(OWN, 8), :], state_out, out_sem.at[0])
    out_total = pltpu.make_async_copy(TOT, coupled_out, out_sem.at[1])
    out_flux = pltpu.make_async_copy(FLUX, coupled_out, out_sem.at[1])

    @pl.when(is_ice)
    def ice():
        both(lambda d: state_copy(d, 0, init), "start")
        loads[1].wait()
        loads[2].wait()
        loads[3].wait()
        cov = COV[...].astype(jnp.float32)
        inv = cov / (4.0 * F[0] + 1.0)
        T[0, :, pl.ds(OWN, 8), :] = F[1] * cov * (1.0 / 3.0)
        T[1, :, pl.ds(OWN, 8), :] = inv
        for x in range(2):
            T[2 + x, :, pl.ds(OWN, 8), :] = inv * (F[2 + x] + CUR[x, :, pl.ds(OWN, 8), :])
        both(ice_static_copy, "start")
        loads[0].wait()
        both(ice_static_copy, "recv")
        for lo in (0, 8, 16):
            inv = T[1, :, pl.ds(lo, 8), :]
            T[4, :, pl.ds(lo, 8), :] = jnp.where(inv > 0.0, 1.0 - inv, 0.0)

        def stress(q, s):
            vx_lo, vx_hi = S[q, 0, :, pl.ds(s - 1, 8), :], S[q, 0, :, pl.ds(s + 1, 8), :]
            vy_lo, vy_hi = S[q, 1, :, pl.ds(s - 1, 8), :], S[q, 1, :, pl.ds(s + 1, 8), :]
            a = vx_hi - vx_lo
            c = dcol(S[q, 1, :, pl.ds(s, 8), :])
            sh = dcol(S[q, 0, :, pl.ds(s, 8), :]) + (vy_hi - vy_lo)
            dd = a + c
            tt = a - c
            p = T[0, :, pl.ds(s, 8), :]
            w = p * lax.rsqrt(4.0 * (dd * dd) + (tt * tt + sh * sh) + 0.16)
            third = 2.0 / 3.0
            S[q, 2, :, pl.ds(s, 8), :] = third * S[q, 2, :, pl.ds(s, 8), :] + (2.0 * (w * dd) - p)
            S[q, 3, :, pl.ds(s, 8), :] = third * S[q, 3, :, pl.ds(s, 8), :] + 0.5 * (w * tt)
            S[q, 4, :, pl.ds(s, 8), :] = third * S[q, 4, :, pl.ds(s, 8), :] + 0.25 * (w * sh)

        def velocity(q, s, to):
            def at(f, o):
                return S[q, f, :, pl.ds(s + o, 8), :]
            fx = 0.25 * ((at(2, 1) + at(3, 1)) - (at(2, -1) + at(3, -1))) + 0.5 * dcol(at(4, 0))
            fy = 0.5 * (at(4, 1) - at(4, -1)) + 0.25 * dcol(at(2, 0) - at(3, 0))
            vx, vy = at(0, 0), at(1, 0)
            ca, cb = T[4, :, pl.ds(s, 8), :], T[1, :, pl.ds(s, 8), :]
            S[to, 0, :, pl.ds(s, 8), :] = ca * (vx + 0.1 * vy) + cb * fx + T[2, :, pl.ds(s, 8), :]
            S[to, 1, :, pl.ds(s, 8), :] = ca * (vy - 0.1 * vx) + cb * fy + T[3, :, pl.ds(s, 8), :]

        def add_total(q):
            vx, vy = S[q, 0, :, pl.ds(OWN, 8), :], S[q, 1, :, pl.ds(OWN, 8), :]
            TOT[0] += vx
            TOT[1] += vy
            TOT[2] += jnp.sqrt(1.0 + vx * vx + vy * vy)

        def phase(p, carry):
            q = lax.rem(p, 2)
            o = 1 - q
            both(lambda d: state_copy(d, q), "recv")
            both(lambda d: state_copy(d, q), "sent")

            @pl.when(p < 2)
            def _():
                pl.semaphore_signal(gate, inc=1, device_id=(1, b), device_id_type=MESH)

            for t, (ss, vs) in enumerate((((1, 9, 17), (2, 10, 18)), ((3, 11, 19), (4, 12)),
                                          ((5, 13), (6, 14)), ((7, 15), (8,)))):
                for s in ss:
                    stress(q, s)
                for s in vs:
                    velocity(q, s, o if t == 3 else q)
                if t == 3:
                    for f in (2, 3, 4):
                        S[o, f, :, pl.ds(OWN, 8), :] = S[q, f, :, pl.ds(OWN, 8), :]
                    @pl.when(p < 3)
                    def _():
                        both(lambda d: state_copy(d, o), "start")
                add_total(o if t == 3 else q)
            return carry

        lax.fori_loop(0, 4, phase, 0)
        both(ice_static_copy, "sent")
        out_state.start()
        cov = COV[...].astype(jnp.float32)
        for x in range(2):
            TOT[x] = TOT[x] * (1.0 / 16.0) - cov * CUR[x, :, pl.ds(OWN, 8), :]
        TOT[2] = TOT[2] * (cov * F[4] * (1.0 / 16.0))
        avg_copy.start()
        out_total.start()
        loads[4].wait()
        loads[5].wait()
        scatter(TOT, 8)
        win_copy.start()
        avg_copy.wait_send()
        out_state.wait()
        out_total.wait()
        win_copy.wait_send()

    @pl.when(jnp.logical_not(is_ice))
    def ocean():
        loads[2].wait()
        pl.semaphore_wait(gate, 1)
        both(lambda d: state_copy(d, 0, init), "start")
        both(ocean_static_copy, "start")
        loads[0].wait()
        loads[1].wait()
        loads[3].wait()
        both(ocean_static_copy, "recv")

        def level(src, dst, l, s, flow):
            px, nx, py, ny = flow
            q = src[l, :, pl.ds(s, 8), :]
            lft, rgt = left_of(q), right_of(q)
            ch = (px * (q - src[l, :, pl.ds(s - 1, 8), :]) + nx * (src[l, :, pl.ds(s + 1, 8), :] - q)
                  + py * (q - lft) + ny * (rgt - q))
            dst[l, :, pl.ds(s, 8), :] = q - (0.2 * LEVELS[l]) * ch

        def step(src, dst, starts):
            for s in starts:
                cx, cy = CUR[0, :, pl.ds(s, 8), :], CUR[1, :, pl.ds(s, 8), :]
                flow = (jnp.maximum(cx, 0.0), jnp.minimum(cx, 0.0), jnp.maximum(cy, 0.0), jnp.minimum(cy, 0.0))
                for l in range(5):
                    level(src, dst, l, s, flow)

        def phase(p, carry):
            q = lax.rem(p, 2)
            o = 1 - q

            both(lambda d: state_copy(d, q), "recv")
            both(lambda d: state_copy(d, q), "sent")
            bufs = (S.at[q], W)
            for t in range(8):
                count = 22 - 2 * t
                starts = [1 + t + 8 * g for g in range(-(-count // 8))]
                step(bufs[t % 2], S.at[o] if t == 7 else bufs[(t + 1) % 2], starts)

            @pl.when(p < 1)
            def _():
                pl.semaphore_wait(gate, 1)
                both(lambda d: state_copy(d, o), "start")

            return carry

        lax.fori_loop(0, 2, phase, 0)
        both(ocean_static_copy, "sent")
        loads[4].wait()
        loads[5].wait()
        avg_copy.wait_recv()
        scatter(RECVA, 0)
        win_copy.wait_recv()
        for ch in range(3):
            FLUX[ch] = FLUX[ch] + RECVW[ch]
        S[0, 0, :, pl.ds(OWN, 8), :] = S[0, 0, :, pl.ds(OWN, 8), :] - 0.5 * FLUX[2]
        out_state.start()
        out_flux.start()
        out_state.wait()
        out_flux.wait()


def to_tiles(x):
    lead, cols = x.shape[:-2], x.shape[-1]
    y = x.reshape(lead + (8, cols // LANE, LANE))
    return jnp.swapaxes(y, -3, -2)


def from_tiles(y):
    x = jnp.swapaxes(y, -3, -2)
    return x.reshape(x.shape[:-2] + (x.shape[-2] * LANE,))


def body(n, initial, ice_forcing, ocean_current, ice_cover, targets, weights):
    cols = initial.shape[-1]
    nt = cols // LANE
    f32 = jnp.float32
    own_t = (nt, 8, LANE)
    ext_t = (nt, RB, LANE)
    args = [to_tiles(x) for x in (initial[0], ice_forcing, ocean_current, ice_cover, targets, weights)]
    dma = pltpu.SemaphoreType.DMA
    state, coupled = pl.pallas_call(
        functools.partial(kernel, n, nt),
        out_shape=(jax.ShapeDtypeStruct((5,) + own_t, f32), jax.ShapeDtypeStruct((3,) + own_t, f32)),
        in_specs=[pl.BlockSpec(memory_space=pl.ANY)] * 6,
        out_specs=(pl.BlockSpec(memory_space=pl.ANY),) * 2,
        scratch_shapes=[
            pltpu.VMEM((2, 5) + ext_t, f32),
            pltpu.VMEM((5,) + ext_t, f32),
            pltpu.VMEM((5,) + ext_t, f32),
            pltpu.VMEM((5,) + own_t, f32),
            pltpu.VMEM((2,) + ext_t, f32),
            pltpu.VMEM(own_t, jnp.int32),
            pltpu.VMEM((2,) + own_t, jnp.int32),
            pltpu.VMEM((2,) + own_t, jnp.int32),
            pltpu.VMEM((3,) + own_t, f32),
            pltpu.VMEM((2, 6) + own_t, f32),
            pltpu.VMEM((2,) + own_t, f32),
            pltpu.VMEM((2,) + own_t, f32),
            pltpu.VMEM((384, 256), f32),
            pltpu.VMEM((3,) + own_t, f32),
            pltpu.VMEM((3,) + own_t, f32),
            pltpu.VMEM((3,) + own_t, f32),
            dma((6,)), dma((2, 2)), dma((2, 2)), dma((2,)), dma((2,)),
            dma, dma, dma, dma, dma((2,)), pltpu.SemaphoreType.REGULAR,
        ],
        compiler_params=pltpu.CompilerParams(collective_id=0, has_side_effects=True),
    )(*args)
    return from_tiles(state)[None], from_tiles(coupled)[None]


def solution(mesh):
    placed = (
        P("comp", None, "blk", None),
        P(None, "blk", None),
        P(None, "blk", None),
        P("blk", None),
        P(None, "blk", None),
        P(None, "blk", None),
    )
    return jax.shard_map(
        functools.partial(body, mesh.shape["blk"]),
        mesh=mesh,
        in_specs=placed,
        out_specs=(P("comp", None, "blk", None), P("comp", None, "blk", None)),
        check_vma=False,
    )
```

```python
import functools
import jax
import jax.numpy as jnp
from jax import lax
from jax.experimental import pallas as pl
from jax.experimental.pallas import tpu as pltpu
from jax.sharding import PartitionSpec as P

LEVELS = (1.0, 0.8, 0.6, 0.45, 0.3)
OWN = 8
RB = 32
LANE = 128
CHAINS = 3
MESH = pl.DeviceIdType.MESH
UP, DOWN = 0, 1


def kernel(n, nt, init, forcing, current, cover, targets, weights, state_out, coupled_out,
           S, Q, W, T, F, CUR, COV, TG, WT, TC, TOT, VALS, TH, TL, RHS, ACC, FLUX, RECVW, RECVA,
           load_sem, ice_send, ice_recv, q_send, q_recv, st_send, st_recv, a_send, a_recv, w_send, w_recv,
           out_sem, gate):
    comp = lax.axis_index("comp")
    b = lax.axis_index("blk")
    is_ice = comp == 0
    has_up = b > 0
    has_down = b < n - 1
    nxt = lax.rem(b + 1, n)
    prv = lax.rem(b + n - 1, n)
    step_t = (nt - 1) // CHAINS
    ct = step_t + 1

    barrier = pltpu.get_barrier_semaphore()

    @pl.when(has_up)
    def _():
        pl.semaphore_signal(barrier, inc=1, device_id=(comp, b - 1), device_id_type=MESH)

    @pl.when(has_down)
    def _():
        pl.semaphore_signal(barrier, inc=1, device_id=(comp, b + 1), device_id_type=MESH)

    pl.semaphore_signal(barrier, inc=1, device_id=(1 - comp, b), device_id_type=MESH)

    @pl.when(is_ice)
    def _():
        pl.semaphore_signal(barrier, inc=1, device_id=(1, nxt), device_id_type=MESH)

    @pl.when(jnp.logical_not(is_ice))
    def _():
        pl.semaphore_signal(barrier, inc=1, device_id=(0, prv), device_id_type=MESH)

    loads = [
        pltpu.make_async_copy(forcing, F, load_sem.at[0]),
        pltpu.make_async_copy(current, CUR.at[:, :, pl.ds(OWN, 8), :], load_sem.at[1]),
        pltpu.make_async_copy(cover, COV, load_sem.at[2]),
        pltpu.make_async_copy(targets, TG, load_sem.at[3]),
        pltpu.make_async_copy(weights, WT, load_sem.at[4]),
    ]
    ice_loads = [
        pltpu.make_async_copy(init.at[:, pl.ds(step_t * c, ct)], S.at[c, 0, :, :, pl.ds(OWN, 8), :], load_sem.at[5 + c])
        for c in range(CHAINS)
    ]
    ocean_load = pltpu.make_async_copy(init, Q.at[0, :, :, pl.ds(OWN, 8), :], load_sem.at[5])
    for c in loads:
        c.start()

    def zeros(*shape):
        return jnp.zeros(shape + (8, LANE), jnp.float32)

    def zero_rows(lo):
        @pl.when(is_ice)
        def _():
            for c in range(CHAINS):
                for q in range(2):
                    S[c, q, :, :, pl.ds(lo, 8), :] = zeros(5, ct)
            T[:, :, pl.ds(lo, 8), :] = zeros(5, nt)

        @pl.when(jnp.logical_not(is_ice))
        def _():
            for q in range(2):
                Q[q, :, :, pl.ds(lo, 8), :] = zeros(5, nt)
            CUR[:, :, pl.ds(lo, 8), :] = zeros(2, nt)

    @pl.when(jnp.logical_not(has_up))
    def _():
        zero_rows(0)

    @pl.when(jnp.logical_not(has_down))
    def _():
        zero_rows(16)

    zero_rows(24)

    def remote(src, dst, ss, rs, dev):
        return pltpu.make_async_remote_copy(src_ref=src, dst_ref=dst, send_sem=ss, recv_sem=rs,
                                            device_id=dev, device_id_type=MESH)

    def beside(d):
        return (16, (comp, b - 1)) if d == UP else (0, (comp, b + 1))

    def ice_copy(d, c, q, src=None):
        lo, dev = beside(d)
        src = S.at[c, q, :, :, pl.ds(OWN, 8), :] if src is None else src
        return remote(src, S.at[c, q, :, :, pl.ds(lo, 8), :], ice_send.at[d, c, q], ice_recv.at[d, c, q], dev)

    def ice_first(d, c):
        return ice_copy(d, c, 0, init.at[:, pl.ds(step_t * c, ct)])

    def ice_static_copy(d, c):
        lo, dev = beside(d)
        t0 = 0 if c == 0 else step_t * c + 1
        tiles = pl.ds(t0, step_t * c + ct - t0)
        return remote(T.at[pl.ds(0, 4), tiles, pl.ds(OWN, 8), :], T.at[pl.ds(0, 4), tiles, pl.ds(lo, 8), :],
                      st_send.at[d, c], st_recv.at[d, c], dev)

    def ocean_copy(d, q, src=None):
        lo, dev = beside(d)
        src = Q.at[q, :, :, pl.ds(OWN, 8), :] if src is None else src
        return remote(src, Q.at[q, :, :, pl.ds(lo, 8), :], q_send.at[d, q], q_recv.at[d, q], dev)

    def ocean_static_copy(d):
        lo, dev = beside(d)
        return remote(current, CUR.at[:, :, pl.ds(lo, 8), :], st_send.at[d, 0], st_recv.at[d, 0], dev)

    def both(make, what):
        pairs = ((UP, has_up, has_down), (DOWN, has_down, has_up))
        for d, sends, receives in pairs:
            @pl.when(receives if what == "recv" else sends)
            def _():
                c = make(d)
                if what == "start":
                    c.start()
                elif what == "recv":
                    c.wait_recv()
                else:
                    c.wait_send()

    zt = zeros(1)

    def lanes(x):
        return lax.broadcasted_iota(jnp.int32, x.shape, 2)

    def right_of(x):
        u = pltpu.roll(x, LANE - 1, 2)
        return jnp.where(lanes(x) == LANE - 1, jnp.concatenate([u[1:], zt], 0), u)

    def left_of(x):
        u = pltpu.roll(x, 1, 2)
        return jnp.where(lanes(x) == 0, jnp.concatenate([zt, u[:-1]], 0), u)

    def dcol(x):
        return right_of(x) - left_of(x)

    avg_copy = remote(TOT, RECVA, a_send, a_recv, (1, b))
    win_copy = remote(FLUX, RECVW, w_send, w_recv, (1, nxt))

    iota = lax.broadcasted_iota(jnp.int32, (16, LANE), 0).astype(jnp.float32)
    iotas = [(iota + 16.0 * g).astype(jnp.bfloat16) for g in range(16)]
    zero = jnp.zeros((16, LANE), jnp.bfloat16)
    one = jnp.ones((16, LANE), jnp.bfloat16)

    def rows16(ref, k, *idx):
        return jnp.broadcast_to(ref[(k,) + idx], (16, LANE)).astype(jnp.bfloat16)

    def plan(base):
        loads[3].wait()
        loads[4].wait()
        for k in range(2):
            t = TG[k]
            row = lax.shift_right_logical(t, 11) - base
            cell = lax.bitwise_and(lax.shift_right_logical(t, 8), 7) * 8 + row
            inside = jnp.logical_and(row >= 0, row < 8)
            TH[k] = jnp.where(inside, cell, 255).astype(jnp.float32)
            TL[k] = lax.bitwise_and(t, 255).astype(jnp.float32)

        def build(i, carry):
            k = i // 8
            r = i % 8
            for j in range(nt):
                tl = rows16(TL, k, j, pl.ds(r, 1), slice(None))
                for g in range(16):
                    RHS[i, pl.ds(16 * g, 16), pl.ds(LANE * j, LANE)] = jnp.where(tl == iotas[g], one, zero)
            return carry

        lax.fori_loop(0, 16, build, 0)

    def scatter(avg_ref):
        for k in range(2):
            w = WT[k].astype(jnp.float32) * 0.25
            for ch in range(3):
                v = avg_ref[ch] * w
                hi = v.astype(jnp.bfloat16).astype(jnp.float32)
                VALS[k, 2 * ch] = hi
                VALS[k, 2 * ch + 1] = v - hi
        ACC[...] = jnp.zeros_like(ACC)

        def body(i, carry):
            k = i // 8
            r = i % 8
            total = None
            for jj in range(nt // 2):
                halves = []
                for j in (2 * jj, 2 * jj + 1):
                    th = rows16(TH, k, j, pl.ds(r, 1), slice(None))
                    masks = [th == iotas[g] for g in range(4)]
                    parts = []
                    for m in range(6):
                        v = rows16(VALS, k, m, j, pl.ds(r, 1), slice(None))
                        parts += [jnp.where(masks[g], v, zero) for g in range(4)]
                    halves.append(jnp.concatenate(parts, 0))
                lhs = jnp.concatenate(halves, 1)
                rhs = RHS[i, :, pl.ds(2 * LANE * jj, 2 * LANE)]
                part = lax.dot_general(lhs, rhs, (((1,), (1,)), ((), ())), preferred_element_type=jnp.float32)
                total = part if total is None else total + part
            ACC[...] += total
            return carry

        lax.fori_loop(0, 16, body, 0)
        for ch in range(3):
            for cb in range(nt // 2):
                for h in range(2):
                    FLUX[ch, 2 * cb + h] = (
                        ACC[pl.ds((2 * ch) * 64 + 8 * cb, 8), pl.ds(LANE * h, LANE)]
                        + ACC[pl.ds((2 * ch + 1) * 64 + 8 * cb, 8), pl.ds(LANE * h, LANE)]
                    )

    barrier_count = 2 + has_up.astype(jnp.int32) + has_down.astype(jnp.int32)

    out_state = pltpu.make_async_copy(Q.at[0, :, :, pl.ds(OWN, 8), :], state_out, out_sem.at[0])
    out_total = pltpu.make_async_copy(TOT, coupled_out, out_sem.at[1])
    out_flux = pltpu.make_async_copy(FLUX, coupled_out, out_sem.at[1])

    @pl.when(is_ice)
    def ice():
        for c in ice_loads:
            c.start()
        for c in range(3):
            loads[c].wait()
        cov = COV[...].astype(jnp.float32)
        inv = cov / (4.0 * F[0] + 1.0)
        T[0, :, pl.ds(OWN, 8), :] = F[1] * cov * (1.0 / 3.0)
        T[1, :, pl.ds(OWN, 8), :] = inv
        for x in range(2):
            T[2 + x, :, pl.ds(OWN, 8), :] = inv * (F[2 + x] + CUR[x, :, pl.ds(OWN, 8), :])
        pl.semaphore_wait(barrier, barrier_count)
        for c in range(CHAINS):
            both(lambda d: ice_first(d, c), "start")
            both(lambda d: ice_static_copy(d, c), "start")
        TC[...] = zeros(CHAINS, 3, ct)
        for c in ice_loads:
            c.wait()
        plan(8)

        def stress(c, q, ss):
            def vel(f, s, o):
                return S[c, q, f, :, pl.ds(s + o, 8), :]

            across_y = [dcol(vel(1, s, 0)) for s in ss]
            across_x = [dcol(vel(0, s, 0)) for s in ss]
            for i, s in enumerate(ss):
                a = vel(0, s, 1) - vel(0, s, -1)
                sh = across_x[i] + (vel(1, s, 1) - vel(1, s, -1))
                dd = a + across_y[i]
                tt = a - across_y[i]
                p = T[0, pl.ds(step_t * c, ct), pl.ds(s, 8), :]
                w = p * lax.rsqrt(4.0 * (dd * dd) + (tt * tt + sh * sh) + 0.16)
                third = 2.0 / 3.0
                S[c, q, 2, :, pl.ds(s, 8), :] = third * S[c, q, 2, :, pl.ds(s, 8), :] + (2.0 * (w * dd) - p)
                S[c, q, 3, :, pl.ds(s, 8), :] = third * S[c, q, 3, :, pl.ds(s, 8), :] + 0.5 * (w * tt)
                S[c, q, 4, :, pl.ds(s, 8), :] = third * S[c, q, 4, :, pl.ds(s, 8), :] + 0.25 * (w * sh)

        def velocity(c, q, ss, to):
            def at(f, s, o):
                return S[c, q, f, :, pl.ds(s + o, 8), :]

            def static(f, s):
                return T[f, pl.ds(step_t * c, ct), pl.ds(s, 8), :]

            d12 = [dcol(at(4, s, 0)) for s in ss]
            d22 = [dcol(at(2, s, 0) - at(3, s, 0)) for s in ss]
            for i, s in enumerate(ss):
                fx = 0.25 * ((at(2, s, 1) + at(3, s, 1)) - (at(2, s, -1) + at(3, s, -1))) + 0.5 * d12[i]
                fy = 0.5 * (at(4, s, 1) - at(4, s, -1)) + 0.25 * d22[i]
                vx, vy = at(0, s, 0), at(1, s, 0)
                ca, cb = static(4, s), static(1, s)
                S[c, to, 0, :, pl.ds(s, 8), :] = ca * (vx + 0.1 * vy) + cb * fx + static(2, s)
                S[c, to, 1, :, pl.ds(s, 8), :] = ca * (vy - 0.1 * vx) + cb * fy + static(3, s)

        def add_total(c, q):
            vx, vy = S[c, q, 0, :, pl.ds(OWN, 8), :], S[c, q, 1, :, pl.ds(OWN, 8), :]
            TC[c, 0] += vx
            TC[c, 1] += vy
            TC[c, 2] += jnp.sqrt(1.0 + vx * vx + vy * vy)

        def turn(i, carry):
            p = i // CHAINS
            c = i % CHAINS
            q = lax.rem(p, 2)
            o = 1 - q
            both(lambda d: ice_copy(d, c, q), "recv")

            @pl.when(i < CHAINS)
            def _():
                for x in range(CHAINS):
                    @pl.when(c == x)
                    def _():
                        both(lambda d: ice_static_copy(d, x), "recv")

                for lo in (0, 8, 16):
                    inv = T[1, pl.ds(step_t * c, ct), pl.ds(lo, 8), :]
                    T[4, pl.ds(step_t * c, ct), pl.ds(lo, 8), :] = jnp.where(inv > 0.0, 1.0 - inv, 0.0)

            both(lambda d: ice_copy(d, c, q), "sent")

            @pl.when(jnp.logical_and(c == CHAINS - 1, p < 2))
            def _():
                pl.semaphore_signal(gate, inc=1, device_id=(1, b), device_id_type=MESH)

            for t, (ss, vs) in enumerate((((1, 9, 17), (2, 10, 18)), ((3, 11, 19), (4, 12)),
                                          ((5, 13), (6, 14)), ((7, 15), (8,)))):
                stress(c, q, ss)
                velocity(c, q, vs, o if t == 3 else q)
                if t == 3:
                    for f in (2, 3, 4):
                        S[c, o, f, :, pl.ds(OWN, 8), :] = S[c, q, f, :, pl.ds(OWN, 8), :]
                    @pl.when(p < 3)
                    def _():
                        both(lambda d: ice_copy(d, c, o), "start")
                add_total(c, o if t == 3 else q)
            return carry

        lax.fori_loop(0, 4 * CHAINS, turn, 0)
        for c in range(CHAINS):
            both(lambda d: ice_static_copy(d, c), "sent")

        def merge(pick, put):
            for c in range(CHAINS):
                v = pick(c)
                put(slice(step_t * c + 1, step_t * c + ct - 1), v[..., 1:-1, :, :])
                if c == 0:
                    put(slice(0, 1), v[..., :1, :, :])
                else:
                    edge = v[..., :1, :, :]
                    left = lax.broadcasted_iota(jnp.int32, edge.shape, edge.ndim - 1) < LANE // 2
                    put(slice(step_t * c, step_t * c + 1), jnp.where(left, before, edge))
                before = v[..., ct - 1 :, :, :]
            put(slice(step_t * CHAINS, step_t * CHAINS + 1), before)

        for x in range(3):
            def put_total(tiles, v):
                cov = COV[tiles].astype(jnp.float32)
                if x < 2:
                    TOT[x, tiles] = v * (1.0 / 16.0) - cov * CUR[x, tiles, pl.ds(OWN, 8), :]
                else:
                    TOT[x, tiles] = v * (cov * F[4, tiles] * (1.0 / 16.0))

            merge(lambda c: TC[c, x], put_total)
        avg_copy.start()
        out_total.start()
        for f in range(5):
            def put_state(tiles, v):
                Q[0, f, tiles, pl.ds(OWN, 8), :] = v

            merge(lambda c: S[c, 0, f, :, pl.ds(OWN, 8), :], put_state)
        out_state.start()
        scatter(TOT)
        win_copy.start()
        avg_copy.wait_send()
        out_state.wait()
        out_total.wait()
        win_copy.wait_send()

    @pl.when(jnp.logical_not(is_ice))
    def ocean():
        ocean_load.start()
        pl.semaphore_wait(barrier, barrier_count)
        plan(0)
        W[:, :, pl.ds(0, 8), :] = zeros(5, nt)
        W[:, :, pl.ds(24, 8), :] = zeros(5, nt)
        for c in range(3):
            loads[c].wait()
        ocean_load.wait()
        pl.semaphore_wait(gate, 1)
        both(lambda d: ocean_copy(d, 0, init), "start")
        both(ocean_static_copy, "start")
        both(ocean_static_copy, "recv")

        def level(src, dst, l, s, flow):
            px, nx, py, ny = flow
            q = src[l, :, pl.ds(s, 8), :]
            lft, rgt = left_of(q), right_of(q)
            ch = (px * (q - src[l, :, pl.ds(s - 1, 8), :]) + nx * (src[l, :, pl.ds(s + 1, 8), :] - q)
                  + py * (q - lft) + ny * (rgt - q))
            dst[l, :, pl.ds(s, 8), :] = q - (0.2 * LEVELS[l]) * ch

        def step(src, dst, starts):
            for s in starts:
                cx, cy = CUR[0, :, pl.ds(s, 8), :], CUR[1, :, pl.ds(s, 8), :]
                flow = (jnp.maximum(cx, 0.0), jnp.minimum(cx, 0.0), jnp.maximum(cy, 0.0), jnp.minimum(cy, 0.0))
                for l in range(5):
                    level(src, dst, l, s, flow)

        def phase(p, carry):
            q = lax.rem(p, 2)
            o = 1 - q

            both(lambda d: ocean_copy(d, q), "recv")
            both(lambda d: ocean_copy(d, q), "sent")
            bufs = (Q.at[q], W)
            for t in range(8):
                count = 22 - 2 * t
                starts = [1 + t + 8 * g for g in range(-(-count // 8))]
                step(bufs[t % 2], Q.at[o] if t == 7 else bufs[(t + 1) % 2], starts)

            @pl.when(p < 1)
            def _():
                pl.semaphore_wait(gate, 1)
                both(lambda d: ocean_copy(d, o), "start")

            return carry

        lax.fori_loop(0, 2, phase, 0)
        both(ocean_static_copy, "sent")
        avg_copy.wait_recv()
        scatter(RECVA)
        win_copy.wait_recv()
        for ch in range(3):
            FLUX[ch] = FLUX[ch] + RECVW[ch]
        Q[0, 0, :, pl.ds(OWN, 8), :] = Q[0, 0, :, pl.ds(OWN, 8), :] - 0.5 * FLUX[2]
        out_state.start()
        out_flux.start()
        out_state.wait()
        out_flux.wait()


def to_tiles(x):
    lead, cols = x.shape[:-2], x.shape[-1]
    y = x.reshape(lead + (8, cols // LANE, LANE))
    return jnp.swapaxes(y, -3, -2)


def from_tiles(y):
    x = jnp.swapaxes(y, -3, -2)
    return x.reshape(x.shape[:-2] + (x.shape[-2] * LANE,))


def body(n, initial, ice_forcing, ocean_current, ice_cover, targets, weights):
    cols = initial.shape[-1]
    nt = cols // LANE
    f32 = jnp.float32
    own_t = (nt, 8, LANE)
    ext_t = (nt, RB, LANE)
    ct = (nt - 1) // CHAINS + 1
    args = [to_tiles(x) for x in (initial[0], ice_forcing, ocean_current, ice_cover, targets, weights)]
    dma = pltpu.SemaphoreType.DMA
    state, coupled = pl.pallas_call(
        functools.partial(kernel, n, nt),
        out_shape=(jax.ShapeDtypeStruct((5,) + own_t, f32), jax.ShapeDtypeStruct((3,) + own_t, f32)),
        in_specs=[pl.BlockSpec(memory_space=pl.ANY)] * 6,
        out_specs=(pl.BlockSpec(memory_space=pl.ANY),) * 2,
        scratch_shapes=[
            pltpu.VMEM((CHAINS, 2, 5, ct, RB, LANE), f32),
            pltpu.VMEM((2, 5) + ext_t, f32),
            pltpu.VMEM((5,) + ext_t, f32),
            pltpu.VMEM((5,) + ext_t, f32),
            pltpu.VMEM((5,) + own_t, f32),
            pltpu.VMEM((2,) + ext_t, f32),
            pltpu.VMEM(own_t, jnp.int32),
            pltpu.VMEM((2,) + own_t, jnp.int32),
            pltpu.VMEM((2,) + own_t, jnp.int32),
            pltpu.VMEM((CHAINS, 3, ct, 8, LANE), f32),
            pltpu.VMEM((3,) + own_t, f32),
            pltpu.VMEM((2, 6) + own_t, f32),
            pltpu.VMEM((2,) + own_t, f32),
            pltpu.VMEM((2,) + own_t, f32),
            pltpu.VMEM((16, 256, cols), jnp.bfloat16),
            pltpu.VMEM((384, 256), f32),
            pltpu.VMEM((3,) + own_t, f32),
            pltpu.VMEM((3,) + own_t, f32),
            pltpu.VMEM((3,) + own_t, f32),
            dma((5 + CHAINS,)), dma((2, CHAINS, 2)), dma((2, CHAINS, 2)), dma((2, 2)), dma((2, 2)),
            dma((2, CHAINS)), dma((2, CHAINS)),
            dma, dma, dma, dma, dma((2,)), pltpu.SemaphoreType.REGULAR,
        ],
        compiler_params=pltpu.CompilerParams(collective_id=0, has_side_effects=True),
    )(*args)
    return from_tiles(state)[None], from_tiles(coupled)[None]


def solution(mesh):
    placed = (
        P("comp", None, "blk", None),
        P(None, "blk", None),
        P(None, "blk", None),
        P("blk", None),
        P(None, "blk", None),
        P(None, "blk", None),
    )
    return jax.shard_map(
        functools.partial(body, mesh.shape["blk"]),
        mesh=mesh,
        in_specs=placed,
        out_specs=(P("comp", None, "blk", None), P("comp", None, "blk", None)),
        check_vma=False,
    )
```

```python
import functools
import jax
import jax.numpy as jnp
from jax import lax
from jax.experimental import pallas as pl
from jax.experimental.pallas import tpu as pltpu
from jax.sharding import PartitionSpec as P

LEVELS = (1.0, 0.8, 0.6, 0.45, 0.3)
OWN = 8
RB = 32
LANE = 128
CHAINS = 3
MESH = pl.DeviceIdType.MESH
UP, DOWN = 0, 1


def kernel(n, nt, init, forcing, current, cover, targets, weights, state_out, coupled_out,
           S, Q, W, T, F, CUR, COV, TG, WT, TC, TOT, VALS, TH, TL, RHS, ACC, FLUX, RECVW, RECVA,
           load_sem, ice_send, ice_recv, st_send, st_recv, a_send, a_recv, w_send, w_recv,
           out_sem, gate):
    comp = lax.axis_index("comp")
    b = lax.axis_index("blk")
    is_ice = comp == 0
    has_up = b > 0
    has_down = b < n - 1
    nxt = lax.rem(b + 1, n)
    prv = lax.rem(b + n - 1, n)
    step_t = (nt - 1) // CHAINS
    ct = step_t + 1

    barrier = pltpu.get_barrier_semaphore()

    @pl.when(has_up)
    def _():
        pl.semaphore_signal(barrier, inc=1, device_id=(comp, b - 1), device_id_type=MESH)

    @pl.when(has_down)
    def _():
        pl.semaphore_signal(barrier, inc=1, device_id=(comp, b + 1), device_id_type=MESH)

    pl.semaphore_signal(barrier, inc=1, device_id=(1 - comp, b), device_id_type=MESH)

    @pl.when(is_ice)
    def _():
        pl.semaphore_signal(barrier, inc=1, device_id=(1, nxt), device_id_type=MESH)

    @pl.when(jnp.logical_not(is_ice))
    def _():
        pl.semaphore_signal(barrier, inc=1, device_id=(0, prv), device_id_type=MESH)

    loads = [
        pltpu.make_async_copy(forcing, F, load_sem.at[0]),
        pltpu.make_async_copy(current, CUR.at[:, :, pl.ds(OWN, 8), :], load_sem.at[1]),
        pltpu.make_async_copy(cover, COV, load_sem.at[2]),
        pltpu.make_async_copy(targets, TG, load_sem.at[3]),
        pltpu.make_async_copy(weights, WT, load_sem.at[4]),
    ]
    ice_loads = [
        pltpu.make_async_copy(init.at[:, pl.ds(step_t * c, ct)], S.at[c, 0, :, :, pl.ds(OWN, 8), :], load_sem.at[5 + c])
        for c in range(CHAINS)
    ]
    for c in loads:
        c.start()

    def zeros(*shape):
        return jnp.zeros(shape + (8, LANE), jnp.float32)

    def zero_rows(lo):
        for c in range(CHAINS):
            for q in range(2):
                S[c, q, :, :, pl.ds(lo, 8), :] = zeros(5, ct)
        T[:, :, pl.ds(lo, 8), :] = zeros(5, nt)
        CUR[:, :, pl.ds(lo, 8), :] = zeros(2, nt)

    @pl.when(jnp.logical_not(has_up))
    def _():
        zero_rows(0)

    @pl.when(jnp.logical_not(has_down))
    def _():
        zero_rows(16)

    zero_rows(24)

    def remote(src, dst, ss, rs, dev):
        return pltpu.make_async_remote_copy(src_ref=src, dst_ref=dst, send_sem=ss, recv_sem=rs,
                                            device_id=dev, device_id_type=MESH)

    def beside(d):
        return (16, (comp, b - 1)) if d == UP else (0, (comp, b + 1))

    def ice_copy(d, c, q, src=None):
        lo, dev = beside(d)
        src = S.at[c, q, :, :, pl.ds(OWN, 8), :] if src is None else src
        return remote(src, S.at[c, q, :, :, pl.ds(lo, 8), :], ice_send.at[d, c, q], ice_recv.at[d, c, q], dev)

    def ice_first(d, c):
        return ice_copy(d, c, 0, init.at[:, pl.ds(step_t * c, ct)])

    def ice_static_copy(d, c):
        lo, dev = beside(d)
        t0 = 0 if c == 0 else step_t * c + 1
        tiles = pl.ds(t0, step_t * c + ct - t0)
        return remote(T.at[pl.ds(0, 4), tiles, pl.ds(OWN, 8), :], T.at[pl.ds(0, 4), tiles, pl.ds(lo, 8), :],
                      st_send.at[d, c], st_recv.at[d, c], dev)

    def ocean_static_copy(d):
        lo, dev = beside(d)
        return remote(current, CUR.at[:, :, pl.ds(lo, 8), :], st_send.at[d, 0], st_recv.at[d, 0], dev)

    def both(make, what):
        pairs = ((UP, has_up, has_down), (DOWN, has_down, has_up))
        for d, sends, receives in pairs:
            @pl.when(receives if what == "recv" else sends)
            def _():
                c = make(d)
                if what == "start":
                    c.start()
                elif what == "recv":
                    c.wait_recv()
                else:
                    c.wait_send()

    zt = zeros(1)

    def lanes(x):
        return lax.broadcasted_iota(jnp.int32, x.shape, 2)

    def right_of(x):
        u = pltpu.roll(x, LANE - 1, 2)
        return jnp.where(lanes(x) == LANE - 1, jnp.concatenate([u[1:], zt], 0), u)

    def left_of(x):
        u = pltpu.roll(x, 1, 2)
        return jnp.where(lanes(x) == 0, jnp.concatenate([zt, u[:-1]], 0), u)

    def dcol(x):
        return right_of(x) - left_of(x)

    avg_copy = remote(TOT, RECVA, a_send, a_recv, (1, b))
    win_copy = remote(FLUX, RECVW, w_send, w_recv, (1, nxt))

    iota = lax.broadcasted_iota(jnp.int32, (16, LANE), 0).astype(jnp.float32)
    iotas = [(iota + 16.0 * g).astype(jnp.bfloat16) for g in range(16)]
    zero = jnp.zeros((16, LANE), jnp.bfloat16)
    one = jnp.ones((16, LANE), jnp.bfloat16)

    def rows16(ref, k, *idx):
        return jnp.broadcast_to(ref[(k,) + idx], (16, LANE)).astype(jnp.bfloat16)

    def plan(base):
        loads[3].wait()
        loads[4].wait()
        for k in range(2):
            t = TG[k]
            row = lax.shift_right_logical(t, 11) - base
            cell = lax.bitwise_and(lax.shift_right_logical(t, 8), 7) * 8 + row
            inside = jnp.logical_and(row >= 0, row < 8)
            TH[k] = jnp.where(inside, cell, 255).astype(jnp.float32)
            TL[k] = lax.bitwise_and(t, 255).astype(jnp.float32)

        def build(i, carry):
            k = i // 8
            r = i % 8
            for j in range(nt):
                tl = rows16(TL, k, j, pl.ds(r, 1), slice(None))
                hot = [jnp.where(tl == iotas[g], one, zero) for g in range(16)]
                RHS[i, :, pl.ds(LANE * j, LANE)] = jnp.concatenate(hot, 0)
            return carry

        lax.fori_loop(0, 16, build, 0)

    def scatter(avg_ref):
        for k in range(2):
            w = WT[k].astype(jnp.float32) * 0.25
            for ch in range(3):
                v = avg_ref[ch] * w
                hi = v.astype(jnp.bfloat16).astype(jnp.float32)
                VALS[k, 2 * ch] = hi
                VALS[k, 2 * ch + 1] = v - hi
        ACC[...] = jnp.zeros_like(ACC)

        def body(r, carry):
            total = None
            for k in range(2):
                for jj in range(nt // 2):
                    halves = []
                    for j in (2 * jj, 2 * jj + 1):
                        th = rows16(TH, k, j, pl.ds(r, 1), slice(None))
                        masks = [th == iotas[g] for g in range(4)]
                        parts = []
                        for m in range(6):
                            v = rows16(VALS, k, m, j, pl.ds(r, 1), slice(None))
                            parts += [jnp.where(masks[g], v, zero) for g in range(4)]
                        halves.append(jnp.concatenate(parts, 0))
                    lhs = jnp.concatenate(halves, 1)
                    rhs = RHS[8 * k + r, :, pl.ds(2 * LANE * jj, 2 * LANE)]
                    part = lax.dot_general(lhs, rhs, (((1,), (1,)), ((), ())), preferred_element_type=jnp.float32)
                    total = part if total is None else total + part
            ACC[...] += total
            return carry

        lax.fori_loop(0, 8, body, 0)
        for ch in range(3):
            for cb in range(nt // 2):
                for h in range(2):
                    FLUX[ch, 2 * cb + h] = (
                        ACC[pl.ds((2 * ch) * 64 + 8 * cb, 8), pl.ds(LANE * h, LANE)]
                        + ACC[pl.ds((2 * ch + 1) * 64 + 8 * cb, 8), pl.ds(LANE * h, LANE)]
                    )

    barrier_count = 2 + has_up.astype(jnp.int32) + has_down.astype(jnp.int32)

    out_state = pltpu.make_async_copy(Q, state_out, out_sem.at[0])
    out_total = pltpu.make_async_copy(TOT, coupled_out, out_sem.at[1])
    out_flux = pltpu.make_async_copy(FLUX, coupled_out, out_sem.at[1])

    def merge(pick, put):
        for c in range(CHAINS):
            v = pick(c)
            put(slice(step_t * c + 1, step_t * c + ct - 1), v[..., 1:-1, :, :])
            if c == 0:
                put(slice(0, 1), v[..., :1, :, :])
            else:
                edge = v[..., :1, :, :]
                left = lax.broadcasted_iota(jnp.int32, edge.shape, edge.ndim - 1) < LANE // 2
                put(slice(step_t * c, step_t * c + 1), jnp.where(left, before, edge))
            before = v[..., ct - 1 :, :, :]
        put(slice(step_t * CHAINS, step_t * CHAINS + 1), before)

    def merge_state():
        for f in range(5):
            def put_state(tiles, v):
                Q[f, tiles] = v

            merge(lambda c: S[c, 0, f, :, pl.ds(OWN, 8), :], put_state)

    @pl.when(is_ice)
    def ice():
        for c in ice_loads:
            c.start()
        for c in range(3):
            loads[c].wait()
        cov = COV[...].astype(jnp.float32)
        inv = cov / (4.0 * F[0] + 1.0)
        T[0, :, pl.ds(OWN, 8), :] = F[1] * cov * (1.0 / 3.0)
        T[1, :, pl.ds(OWN, 8), :] = inv
        for x in range(2):
            T[2 + x, :, pl.ds(OWN, 8), :] = inv * (F[2 + x] + CUR[x, :, pl.ds(OWN, 8), :])
        pl.semaphore_wait(barrier, barrier_count)
        for c in range(CHAINS):
            both(lambda d: ice_first(d, c), "start")
            both(lambda d: ice_static_copy(d, c), "start")
        TC[...] = zeros(CHAINS, 3, ct)
        for c in ice_loads:
            c.wait()
        plan(8)

        def stress(c, q, ss):
            def vel(f, s, o):
                return S[c, q, f, :, pl.ds(s + o, 8), :]

            across_y = [dcol(vel(1, s, 0)) for s in ss]
            across_x = [dcol(vel(0, s, 0)) for s in ss]
            for i, s in enumerate(ss):
                a = vel(0, s, 1) - vel(0, s, -1)
                sh = across_x[i] + (vel(1, s, 1) - vel(1, s, -1))
                dd = a + across_y[i]
                tt = a - across_y[i]
                p = T[0, pl.ds(step_t * c, ct), pl.ds(s, 8), :]
                w = p * lax.rsqrt(4.0 * (dd * dd) + (tt * tt + sh * sh) + 0.16)
                third = 2.0 / 3.0
                S[c, q, 2, :, pl.ds(s, 8), :] = third * S[c, q, 2, :, pl.ds(s, 8), :] + (2.0 * (w * dd) - p)
                S[c, q, 3, :, pl.ds(s, 8), :] = third * S[c, q, 3, :, pl.ds(s, 8), :] + 0.5 * (w * tt)
                S[c, q, 4, :, pl.ds(s, 8), :] = third * S[c, q, 4, :, pl.ds(s, 8), :] + 0.25 * (w * sh)

        def velocity(c, q, ss, to):
            def at(f, s, o):
                return S[c, q, f, :, pl.ds(s + o, 8), :]

            def static(f, s):
                return T[f, pl.ds(step_t * c, ct), pl.ds(s, 8), :]

            d12 = [dcol(at(4, s, 0)) for s in ss]
            d22 = [dcol(at(2, s, 0) - at(3, s, 0)) for s in ss]
            for i, s in enumerate(ss):
                fx = 0.25 * ((at(2, s, 1) + at(3, s, 1)) - (at(2, s, -1) + at(3, s, -1))) + 0.5 * d12[i]
                fy = 0.5 * (at(4, s, 1) - at(4, s, -1)) + 0.25 * d22[i]
                vx, vy = at(0, s, 0), at(1, s, 0)
                ca, cb = static(4, s), static(1, s)
                S[c, to, 0, :, pl.ds(s, 8), :] = ca * (vx + 0.1 * vy) + cb * fx + static(2, s)
                S[c, to, 1, :, pl.ds(s, 8), :] = ca * (vy - 0.1 * vx) + cb * fy + static(3, s)

        def add_total(c, q):
            vx, vy = S[c, q, 0, :, pl.ds(OWN, 8), :], S[c, q, 1, :, pl.ds(OWN, 8), :]
            TC[c, 0] += vx
            TC[c, 1] += vy
            TC[c, 2] += jnp.sqrt(1.0 + vx * vx + vy * vy)

        def turn(i, carry):
            p = i // CHAINS
            c = i % CHAINS
            q = lax.rem(p, 2)
            o = 1 - q
            both(lambda d: ice_copy(d, c, q), "recv")

            @pl.when(i < CHAINS)
            def _():
                for x in range(CHAINS):
                    @pl.when(c == x)
                    def _():
                        both(lambda d: ice_static_copy(d, x), "recv")

                for lo in (0, 8, 16):
                    inv = T[1, pl.ds(step_t * c, ct), pl.ds(lo, 8), :]
                    T[4, pl.ds(step_t * c, ct), pl.ds(lo, 8), :] = jnp.where(inv > 0.0, 1.0 - inv, 0.0)

            both(lambda d: ice_copy(d, c, q), "sent")

            @pl.when(i == 2)
            def _():
                pl.semaphore_signal(gate, inc=1, device_id=(1, b), device_id_type=MESH)

            for t, (ss, vs) in enumerate((((1, 9, 17), (2, 10, 18)), ((3, 11, 19), (4, 12)),
                                          ((5, 13), (6, 14)), ((7, 15), (8,)))):
                stress(c, q, ss)
                velocity(c, q, vs, o if t == 3 else q)
                if t == 3:
                    for f in (2, 3, 4):
                        S[c, o, f, :, pl.ds(OWN, 8), :] = S[c, q, f, :, pl.ds(OWN, 8), :]
                    @pl.when(p < 3)
                    def _():
                        both(lambda d: ice_copy(d, c, o), "start")
                add_total(c, o if t == 3 else q)
            return carry

        lax.fori_loop(0, 4 * CHAINS, turn, 0)
        for c in range(CHAINS):
            both(lambda d: ice_static_copy(d, c), "sent")

        for x in range(3):
            def put_total(tiles, v):
                cov = COV[tiles].astype(jnp.float32)
                if x < 2:
                    TOT[x, tiles] = v * (1.0 / 16.0) - cov * CUR[x, tiles, pl.ds(OWN, 8), :]
                else:
                    TOT[x, tiles] = v * (cov * F[4, tiles] * (1.0 / 16.0))

            merge(lambda c: TC[c, x], put_total)
        avg_copy.start()
        out_total.start()
        merge_state()
        out_state.start()
        scatter(TOT)
        win_copy.start()
        avg_copy.wait_send()
        out_state.wait()
        out_total.wait()
        win_copy.wait_send()

    @pl.when(jnp.logical_not(is_ice))
    def ocean():
        for c in ice_loads:
            c.start()
        pl.semaphore_wait(barrier, barrier_count)
        plan(0)
        W[:, :, pl.ds(0, 8), :] = zeros(5, ct)
        W[:, :, pl.ds(24, 8), :] = zeros(5, ct)
        for c in range(3):
            loads[c].wait()
        for c in ice_loads:
            c.wait()
        pl.semaphore_wait(gate, 1)
        both(ocean_static_copy, "start")
        for c in range(CHAINS):
            both(lambda d: ice_first(d, c), "start")
        both(ocean_static_copy, "recv")

        def get(c, slot, l, s):
            return W[l, :, pl.ds(s, 8), :] if slot is None else S[c, slot, l, :, pl.ds(s, 8), :]

        def level(c, src, dst, l, s, flow):
            px, nx, py, ny = flow
            q = get(c, src, l, s)
            lft, rgt = left_of(q), right_of(q)
            ch = px * (q - get(c, src, l, s - 1)) + nx * (get(c, src, l, s + 1) - q) + py * (q - lft) + ny * (rgt - q)
            new = q - (0.2 * LEVELS[l]) * ch
            if dst is None:
                W[l, :, pl.ds(s, 8), :] = new
            else:
                S[c, dst, l, :, pl.ds(s, 8), :] = new

        def step(c, src, dst, starts):
            for s in starts:
                cx, cy = (CUR[x, pl.ds(step_t * c, ct), pl.ds(s, 8), :] for x in range(2))
                flow = (jnp.maximum(cx, 0.0), jnp.minimum(cx, 0.0), jnp.maximum(cy, 0.0), jnp.minimum(cy, 0.0))
                for l in range(5):
                    level(c, src, dst, l, s, flow)

        def turn(i, carry):
            p = i // CHAINS
            c = i % CHAINS
            q = lax.rem(p, 2)
            o = 1 - q
            both(lambda d: ice_copy(d, c, q), "recv")
            both(lambda d: ice_copy(d, c, q), "sent")
            slots = (q, None)
            for t in range(8):
                count = 22 - 2 * t
                starts = [1 + t + 8 * g for g in range(-(-count // 8))]
                step(c, slots[t % 2], o if t == 7 else slots[(t + 1) % 2], starts)

            @pl.when(p < 1)
            def _():
                both(lambda d: ice_copy(d, c, o), "start")

            return carry

        lax.fori_loop(0, 2 * CHAINS, turn, 0)
        merge_state()
        both(ocean_static_copy, "sent")
        avg_copy.wait_recv()
        scatter(RECVA)
        win_copy.wait_recv()
        for ch in range(3):
            FLUX[ch] = FLUX[ch] + RECVW[ch]
        Q[0] = Q[0] - 0.5 * FLUX[2]
        out_state.start()
        out_flux.start()
        out_state.wait()
        out_flux.wait()


def to_tiles(x):
    lead, cols = x.shape[:-2], x.shape[-1]
    y = x.reshape(lead + (8, cols // LANE, LANE))
    return jnp.swapaxes(y, -3, -2)


def from_tiles(y):
    x = jnp.swapaxes(y, -3, -2)
    return x.reshape(x.shape[:-2] + (x.shape[-2] * LANE,))


def body(n, initial, ice_forcing, ocean_current, ice_cover, targets, weights):
    cols = initial.shape[-1]
    nt = cols // LANE
    f32 = jnp.float32
    own_t = (nt, 8, LANE)
    ext_t = (nt, RB, LANE)
    ct = (nt - 1) // CHAINS + 1
    args = [to_tiles(x) for x in (initial[0], ice_forcing, ocean_current, ice_cover, targets, weights)]
    dma = pltpu.SemaphoreType.DMA
    state, coupled = pl.pallas_call(
        functools.partial(kernel, n, nt),
        out_shape=(jax.ShapeDtypeStruct((5,) + own_t, f32), jax.ShapeDtypeStruct((3,) + own_t, f32)),
        in_specs=[pl.BlockSpec(memory_space=pl.ANY)] * 6,
        out_specs=(pl.BlockSpec(memory_space=pl.ANY),) * 2,
        scratch_shapes=[
            pltpu.VMEM((CHAINS, 2, 5, ct, RB, LANE), f32),
            pltpu.VMEM((5,) + own_t, f32),
            pltpu.VMEM((5, ct, RB, LANE), f32),
            pltpu.VMEM((5,) + ext_t, f32),
            pltpu.VMEM((5,) + own_t, f32),
            pltpu.VMEM((2,) + ext_t, f32),
            pltpu.VMEM(own_t, jnp.int32),
            pltpu.VMEM((2,) + own_t, jnp.int32),
            pltpu.VMEM((2,) + own_t, jnp.int32),
            pltpu.VMEM((CHAINS, 3, ct, 8, LANE), f32),
            pltpu.VMEM((3,) + own_t, f32),
            pltpu.VMEM((2, 6) + own_t, f32),
            pltpu.VMEM((2,) + own_t, f32),
            pltpu.VMEM((2,) + own_t, f32),
            pltpu.VMEM((16, 256, cols), jnp.bfloat16),
            pltpu.VMEM((384, 256), f32),
            pltpu.VMEM((3,) + own_t, f32),
            pltpu.VMEM((3,) + own_t, f32),
            pltpu.VMEM((3,) + own_t, f32),
            dma((5 + CHAINS,)), dma((2, CHAINS, 2)), dma((2, CHAINS, 2)),
            dma((2, CHAINS)), dma((2, CHAINS)),
            dma, dma, dma, dma, dma((2,)), pltpu.SemaphoreType.REGULAR,
        ],
        compiler_params=pltpu.CompilerParams(collective_id=0, has_side_effects=True),
    )(*args)
    return from_tiles(state)[None], from_tiles(coupled)[None]


def solution(mesh):
    placed = (
        P("comp", None, "blk", None),
        P(None, "blk", None),
        P(None, "blk", None),
        P("blk", None),
        P(None, "blk", None),
        P(None, "blk", None),
    )
    return jax.shard_map(
        functools.partial(body, mesh.shape["blk"]),
        mesh=mesh,
        in_specs=placed,
        out_specs=(P("comp", None, "blk", None), P("comp", None, "blk", None)),
        check_vma=False,
    )
```
